32 devices in a mesh: groups: 2 (over y), tok: 8 (over z, core), head: 2 (over x), pair: 1.
Axes of the slice: x: 2, y: 2, z: 4, core: 2. Of those that a mesh axis runs over, the one named last changes fastest.
Arguments:
- queries: bfloat16 [2048, 4096], P(('groups', 'tok'), ('head', 'pair')), parts along dimension 0, may hold values from -6 to 6
- keys_values: bfloat16 [2048, 1024], P(('groups', 'tok'), ('head', 'pair')), parts along dimension 0, may hold values from -6 to 6
- sink_logits: float32 [64], P(('head', 'pair')), may hold values from -2 to 3
- residual: bfloat16 [2048, 2880], P(('groups', 'tok')), parts along dimension 0, may hold values from -60 to 60
- out_weight: bfloat16 [4096, 2880], P(('head', 'pair')), may hold values from -0.09375 to 0.09375
- norm_gain: float32 [2880], replicated, may hold values from 0.5 to 1.5
- expert_ids: int32 [2048, 4], P(('groups', 'tok')), parts along dimension 0, may hold values from 0 to 7, all different within a row; in each aligned block of 128 rows (0 to 127, 128 to 255, ...) at most 80 rows name the same one
- route_weights: float32 [2048, 4], P(('groups', 'tok')), parts along dimension 0, may hold values from 0.1 to 1
- gate_up: bfloat16 [8, 2880, 2, 1440], P('tok', None, None, ('head', 'pair')), may hold values from -0.109375 to 0.109375
- down_weight: bfloat16 [8, 1440, 2880], P('tok', ('head', 'pair')), may hold values from -0.21875 to 0.21875
Outputs:
- layer_output: bfloat16 [2048, 2880], P(('groups', 'tok'), ('head', 'pair')), parts along dimension 0
The draws below stay inside these ranges and needn't reach their ends.
There are 2 independent parts, one for each index of `groups`. The reference program is written for one: setup_inputs(seed, part) draws one part's arguments, and reference() takes and returns one part's arrays. A program takes and returns all parts, laid end to end along the dimension named above; an argument that names none is the same for every part. Nothing has to cross between parts.
Inputs may be any that keep to these rules, and one draw needn't show every extreme that they name: `expert_ids`: in each aligned block of 128 rows (the rows of one index of tok), a row names 4 different experts and no expert is named by more than 80 rows.
All inputs are finite; a program needn't handle non-finite values.
Results may differ from the reference program's by a relative error of at most 0.01.
Values may be sent and summed in bfloat16 or wider, within the bound.
A program may use at most 128 MiB of HBM per device.

```python
import math
import jax
import jax.numpy as jnp
import numpy as np
from jax import lax

D = 2880
HEADS = 64
KV_HEADS = 8
HEAD_DIM = 64
FFE = 1440
TOP = 4
TOK_DEV = 128
TOKENS = 1024
EXPERTS = 8
CAP = 80
N_TOK = 8


def attention_inputs(key):
    base = jax.random.fold_in(key, 11)
    key_query, key_keys = jax.random.split(base, 2)
    query_width = HEADS * HEAD_DIM
    key_width = KV_HEADS * 2 * HEAD_DIM
    queries = jnp.clip(jax.random.normal(key_query, (TOKENS, query_width), jnp.float32), -6.0, 6.0)
    keys_values = jnp.clip(jax.random.normal(key_keys, (TOKENS, key_width), jnp.float32), -6.0, 6.0)
    return (queries, keys_values)


def draw_queries(key, part):
    return attention_inputs(key)[0].astype(jnp.bfloat16)


def draw_keys_values(key, part):
    return attention_inputs(key)[1].astype(jnp.bfloat16)


def draw_residual(key, part):
    key_base, key_rows, key_cols = jax.random.split(jax.random.fold_in(key, 5), 3)
    values = jnp.clip(jax.random.normal(key_base, (TOKENS, D), jnp.float32), -4.0, 4.0)
    row_scale = jnp.exp(jax.random.uniform(key_rows, (TOKENS, 1), jnp.float32, -1.2, 1.1))
    rising = 0.6 + 1.2 * jnp.arange(D, dtype=jnp.float32)[None, :] / D
    col_scale = jnp.exp(jax.random.uniform(key_cols, (1, D), jnp.float32, -1.0, 1.0)) * rising
    return (values * row_scale * col_scale).astype(jnp.bfloat16)


def strengthened(values, rng, source, target, shards_of, factor):
    def block_of(dim):
        return (jnp.arange(values.shape[dim]) // (values.shape[dim] // shards_of)).reshape((-1,) + (1,) * (values.ndim - 1 - dim))

    near = jax.random.permutation(rng, shards_of)[block_of(target)]
    other_side = (block_of(target) + shards_of // 2) % shards_of
    return jnp.where((block_of(source) == near) | (block_of(source) == other_side), factor * values, values)


def levels(stream_key, extent, cuts, smallest, high):
    def one(dim, shards_of):
        steps = jax.random.uniform(jax.random.fold_in(jax.random.fold_in(stream_key, 6), dim), (shards_of,), jnp.float32, smallest / len(cuts), high / len(cuts))
        return jnp.repeat(jnp.exp(steps), extent[dim] // shards_of).reshape((-1,) + (1,) * (len(extent) - dim - 1))

    factor_of = one(*cuts[0])
    for cut in cuts[1:]:
        factor_of = factor_of * one(*cut)
    return factor_of


def deal_out(rng, own, number, rows, number_of, top, limit, lean):
    sequence = jax.random.permutation(rng, number_of)
    heavy_load, usual = load_shares(number_of, rows * top, limit, lean, True), load_shares(number_of, rows * top, limit, lean, False)
    places = jnp.arange(number_of)

    def named(sizes, rotation):
        used = int((sizes > 0).sum())
        fixed = max(1, used // 4)
        moved = fixed + (places - fixed + rotation * (used - fixed)) % max(1, number_of - fixed)
        return jnp.zeros((number_of,), jnp.int32).at[sequence[jnp.where(places < fixed, places, moved)]].set(jnp.asarray(sizes, jnp.int32))

    sizes = jnp.where(number % 4 == 0, named(heavy_load, number // 4), named(usual, number - number // 4 - 1))
    mixed = jax.random.permutation(jax.random.fold_in(own, 3), number_of)
    source_of, receiver = mixed[0:number_of // 2 * 2:2], mixed[1:number_of // 2 * 2:2]
    slack = jnp.minimum(sizes[source_of] - 1, limit - sizes[receiver]) // 2
    slack = jnp.where((source_of == sequence[0]) | (receiver == sequence[0]) | (sizes[receiver] == 0), 0, jnp.maximum(slack, 0))
    moved = jax.random.randint(jax.random.fold_in(own, 4), (number_of // 2,), 0, 1 << 20) % (slack + 1)
    sizes = sizes.at[source_of].add(-moved).at[receiver].add(moved)
    items = jnp.searchsorted(jnp.cumsum(sizes), jnp.arange(rows * top), side="right").astype(jnp.int32)
    table = items.reshape(top, rows).T
    table = table[jax.random.permutation(jax.random.fold_in(own, 1), rows)]
    rotation = jax.random.randint(jax.random.fold_in(own, 2), (rows, 1), 0, top)
    return jnp.take_along_axis(table, (jnp.arange(top)[None, :] + rotation) % top, axis=1)


def load_shares(count, total, most, lean, full):
    loads = [(1 << 20) // math.isqrt(rank ** lean) + 1 for rank in range(1, count + 1)]
    largest = most if full else min(most, max(-(-total // count), total * loads[0] // sum(loads)))
    least = 1 if total - largest >= count - 1 else 0
    holding, spare = [largest] + [least] * (count - 1), total - largest - least * (count - 1)
    while spare > 0:
        candidates = [i for i in range(1, count) if holding[i] < largest] or [i for i in range(1, count) if holding[i] < most]
        pool, budget = sum([loads[i] for i in candidates]), spare
        for i in candidates:
            extra = min(most - holding[i], max(1, budget * loads[i] // pool), spare)
            holding[i] = holding[i] + extra
            spare = spare - extra
    return np.array(holding)


def noise(key, dims, deviation, bound, pieces=(), kind=jnp.bfloat16):
    values = jax.random.normal(key, dims, jnp.float32) * deviation
    if len(pieces) > 0:
        values = levels(key, dims, pieces, -0.22, 0.18) * values
    return jnp.clip(values, min=-bound, max=bound).astype(kind)


def gaussian_with(rng, extent, spread, limit, shards, heavy, held_as=jnp.bfloat16):
    values = spread * jax.random.normal(rng, extent, jnp.float32)
    if shards:
        values = values * levels(rng, extent, shards, -0.22, 0.18)
    return jnp.clip(strengthened(values, jax.random.fold_in(rng, 3), *heavy), -limit, limit).astype(held_as)


def setup_inputs(seed: int = 0, part: int = 0) -> dict:
    arg_keys = jax.random.split(jax.random.key(seed), 11)
    part_splits = jax.random.split(jax.random.fold_in(arg_keys[10], part), 11)
    queries = draw_queries(jax.random.fold_in(jax.random.fold_in(arg_keys[10], part), 71), part)
    keys_values = draw_keys_values(jax.random.fold_in(jax.random.fold_in(arg_keys[10], part), 71), part)
    sink_logits = jnp.clip(-2.0 + 5.0 * jax.random.uniform(arg_keys[2], (HEADS,), jnp.float32) ** levels(arg_keys[2], (HEADS,), ((0, 2),), -0.2, 0.2), -2.0, 3.0)
    residual = draw_residual(jax.random.fold_in(jax.random.fold_in(arg_keys[10], part), 71), part)
    out_weight = noise(arg_keys[4], (HEADS * HEAD_DIM, D), (HEADS * HEAD_DIM) ** -0.5, 0.09375, ((0, 2),))
    norm_gain = jnp.clip(1.0 + 0.1 * jax.random.normal(arg_keys[5], (D,), jnp.float32), 0.5, 1.5)
    expert_ids_keys = jax.random.split(jax.random.fold_in(part_splits[6], 1), TOKENS // TOK_DEV)
    expert_ids_turns = jax.random.permutation(jax.random.fold_in(part_splits[6], 3), TOKENS // TOK_DEV)
    expert_ids = jax.vmap(lambda own, number: deal_out(jax.random.fold_in(part_splits[6], 2), own, number, TOK_DEV, EXPERTS, TOP, CAP, 2))(expert_ids_keys, expert_ids_turns).reshape((TOKENS, TOP))
    route_weights = jnp.clip(0.1 + 0.9 * jax.random.uniform(part_splits[7], (TOKENS, TOP), jnp.float32) ** levels(part_splits[7], (TOKENS, TOP), ((0, 8),), -0.2, 0.2), 0.1, 1.0)
    gate_up = noise(arg_keys[8], (EXPERTS, D, 2, FFE), D ** -0.5, 0.109375, ((0, 8), (3, 2)))
    down_weight = gaussian_with(arg_keys[9], (EXPERTS, FFE, D), FFE ** -0.5, 0.21875, ((0, 8), (1, 2)), (1, 2, 2, 2.0))
    return {"queries": queries, "keys_values": keys_values, "sink_logits": sink_logits, "residual": residual, "out_weight": out_weight, "norm_gain": norm_gain, "expert_ids": expert_ids, "route_weights": route_weights, "gate_up": gate_up, "down_weight": down_weight}


def slot_places(expert_ids, experts, capacity):
    tok_rows = expert_ids.shape[0]
    fanout = expert_ids.shape[1]
    flat_ids = expert_ids.reshape(-1).astype(jnp.int32)
    one_hot = (flat_ids[:, None] == jnp.arange(experts, dtype=jnp.int32)[None, :]).astype(jnp.int32)
    earlier = (jnp.cumsum(one_hot, axis=0) - one_hot).astype(jnp.int32)
    ranking = lax.optimization_barrier(jnp.sum(earlier * one_hot, axis=1)).astype(jnp.int32)
    targets = (flat_ids * capacity + ranking).astype(jnp.int32)
    sources = jnp.arange(tok_rows * fanout, dtype=jnp.int32) // fanout
    table = jnp.full((experts * capacity,), tok_rows, jnp.int32).at[targets].set(sources)
    return (targets.reshape(tok_rows, fanout), table)

def reference(queries, keys_values, sink_logits, residual, out_weight, norm_gain, expert_ids, route_weights, gate_up, down_weight):
    length = queries.shape[0]
    repeat = HEADS // KV_HEADS
    position = jnp.arange(length, dtype=jnp.int32)
    allowed = position[None, :] <= position[:, None]

    def one_head(number):
        query_head = lax.dynamic_slice_in_dim(queries, number * HEAD_DIM, HEAD_DIM, 1)
        group = number // repeat
        key_head = lax.dynamic_slice_in_dim(keys_values, group * 2 * HEAD_DIM, HEAD_DIM, 1)
        value_head = lax.dynamic_slice_in_dim(keys_values, group * 2 * HEAD_DIM + HEAD_DIM, HEAD_DIM, 1)
        scores = jnp.dot(query_head, key_head.T, preferred_element_type=jnp.float32) * 0.125
        scores = jnp.where(allowed, scores, jnp.float32(-1e+30))
        sink_value = sink_logits[number]
        top_value = jnp.maximum(lax.optimization_barrier(jnp.max(scores, axis=-1)), sink_value)
        weights = jnp.exp(scores - top_value[:, None])
        totals = jnp.exp(sink_value - top_value) + lax.optimization_barrier(jnp.sum(weights, axis=-1))
        mixed = jnp.dot(weights.astype(jnp.bfloat16), value_head, preferred_element_type=jnp.float32)
        return (mixed / totals[:, None]).astype(jnp.bfloat16)
    heads_out = lax.map(one_head, jnp.arange(HEADS, dtype=jnp.int32))
    attended = jnp.transpose(heads_out, (1, 0, 2)).reshape(length, HEADS * HEAD_DIM)
    projected = jnp.dot(attended, out_weight, preferred_element_type=jnp.float32)
    stream = residual.astype(jnp.float32) + projected
    inverse = lax.rsqrt(lax.optimization_barrier(jnp.mean(stream * stream, axis=-1, keepdims=True)) + 1e-05)
    normed = (stream * inverse * norm_gain).astype(jnp.bfloat16)
    block_ids = expert_ids.reshape(N_TOK, TOK_DEV, TOP)
    targets, tables = jax.vmap(lambda block_rows: slot_places(block_rows, EXPERTS, CAP))(block_ids)
    padded = jnp.concatenate([normed.reshape(N_TOK, TOK_DEV, D), jnp.zeros((N_TOK, 1, D), jnp.bfloat16)], axis=1)

    def pick_rows(block_rows, table_row):
        return block_rows[table_row]
    dispatched = jax.vmap(pick_rows)(padded, tables).reshape(N_TOK, EXPERTS, CAP, D)
    dispatched = jnp.transpose(dispatched, (1, 0, 2, 3))

    def one_expert(number):
        inputs = dispatched[number].reshape(N_TOK * CAP, D)
        weights_in = gate_up[number]
        gate_part = jnp.dot(inputs, weights_in[:, 0, :], preferred_element_type=jnp.float32)
        up_part = jnp.dot(inputs, weights_in[:, 1, :], preferred_element_type=jnp.float32)
        active = (gate_part * jax.nn.sigmoid(1.702 * gate_part) * (up_part + 1.0)).astype(jnp.bfloat16)
        result = jnp.dot(active, down_weight[number], preferred_element_type=jnp.float32).astype(jnp.bfloat16)
        return result.reshape(N_TOK, CAP, D)
    expert_out = lax.map(one_expert, jnp.arange(EXPERTS, dtype=jnp.int32))
    ranks = (targets - block_ids * CAP).astype(jnp.int32)
    block_index = jnp.arange(N_TOK, dtype=jnp.int32)[:, None, None]
    picked = expert_out[block_ids, block_index, ranks].reshape(length, TOP, D)
    mixture = lax.optimization_barrier(jnp.sum(route_weights[:, :, None] * picked.astype(jnp.float32), axis=1))
    return (stream + mixture).astype(jnp.bfloat16)
```

```python
import functools

import jax
import jax.numpy as jnp
from jax import lax
from jax.experimental import pallas as pl
from jax.experimental.pallas import tpu as pltpu
from jax.sharding import PartitionSpec as P

HEAD_DIM = 64

MESH_ID = pl.DeviceIdType.MESH


def moe_kernel(
    dims,
    x_ref,
    gate_hbm,
    down_hbm,
    out_ref,
    gate_w,
    down_w,
    rows,
    part,
    from_core,
    kept,
    from_peer,
    hop,
    from_right,
    from_left,
    load_sem,
    row_recv,
    row_right,
    row_left,
    row_peer,
    row_core,
    part_send,
    part_recv,
    peer_send,
    peer_recv,
    hop_send,
    right_recv,
    left_recv,
):
    chips, cores, shares, pairs, width = dims
    tok = lax.axis_index("tok")
    z = tok // cores
    c = tok % cores
    mine = lax.axis_index("head") * pairs + lax.axis_index("pair")
    other = cores - 1 - c

    def tok_id(chip, core):
        return {"tok": chip * cores + core}

    def peer_id(share):
        return {"head": share // pairs, "pair": share % pairs}

    def remote(src, dst, send, recv, target):
        return pltpu.make_async_remote_copy(
            src_ref=src, dst_ref=dst, send_sem=send, recv_sem=recv,
            device_id=target, device_id_type=MESH_ID,
        )

    loads = [
        pltpu.make_async_copy(gate_hbm, gate_w, load_sem.at[0]),
        pltpu.make_async_copy(down_hbm, down_w, load_sem.at[1]),
        pltpu.make_async_copy(x_ref, rows.at[z, mine, c], load_sem.at[2]),
    ]
    for load in loads:
        load.start()

    barrier = pltpu.get_barrier_semaphore()

    @pl.when(z > 0)
    def _():
        pl.semaphore_signal(barrier, 1, device_id=tok_id(z - 1, c), device_id_type=MESH_ID)

    @pl.when(z < chips - 1)
    def _():
        pl.semaphore_signal(barrier, 1, device_id=tok_id(z + 1, c), device_id_type=MESH_ID)

    if cores > 1:
        pl.semaphore_signal(barrier, 1, device_id=tok_id(z, other), device_id_type=MESH_ID)
    for d in range(1, shares):
        pl.semaphore_signal(
            barrier, 1, device_id=peer_id((mine + d) % shares), device_id_type=MESH_ID
        )
    sides = jnp.where(z > 0, 1, 0) + jnp.where(z < chips - 1, 1, 0)
    pl.semaphore_wait(barrier, sides + (cores - 1) + (shares - 1))
    loads[2].wait()

    near = jnp.minimum(z, chips - 1 - z)

    def chip_at(i):
        inner = jnp.where(i % 2 == 1, z - (i + 1) // 2, z + i // 2)
        outer = jnp.where(z < chips - 1 - z, i, chips - 1 - i)
        return jnp.where(i <= 2 * near, inner, outer)

    def row_copy(chip, share, core, send, target):
        slot = rows.at[chip, share, core]
        return remote(slot, slot, send, row_recv.at[chip, core, share], target)

    def go_right(chip):
        return (chip <= z) & (z < chips - 1)

    def go_left(chip):
        return (chip >= z) & (z > 0)

    def right_copy(chip):
        return row_copy(chip, mine, c, row_right.at[chip], tok_id(z + 1, c))

    def left_copy(chip):
        return row_copy(chip, mine, c, row_left.at[chip], tok_id(z - 1, c))

    def peer_copy(chip, d):
        return row_copy(chip, mine, c, row_peer.at[chip, d - 1], peer_id((mine + d) % shares))

    def core_copy(chip, share):
        return row_copy(chip, share, c, row_core.at[chip, share], tok_id(z, other))

    def row_wait(chip, share, core):
        slot = rows.at[chip, share, core]
        pltpu.make_async_copy(slot, slot, row_recv.at[chip, core, share]).wait()

    def forward(i):
        chip = chip_at(i)

        @pl.when(go_right(chip))
        def _():
            right_copy(chip).start()

        @pl.when(go_left(chip))
        def _():
            left_copy(chip).start()

        for d in range(1, shares):
            peer_copy(chip, d).start()
        if cores > 1:
            core_copy(chip, mine).start()

    forward(0)
    loads[0].wait()
    loads[1].wait()

    tail = (width // 128) * 128
    wide = rows.shape[-1]
    depth = rows.shape[-2]
    experts = chips * cores
    tail_lane = tail + lax.broadcasted_iota(jnp.int32, (cores * depth, wide - tail), 1)
    weight_lane = (tail_lane == width + tok) | (tail_lane == width + experts + tok)

    def kept_at(chip, share):
        return kept.at[chip, share] if cores > 1 else part.at[chip, share, 0]

    def part_copy(chip, share):
        return remote(
            part.at[chip, share, other], from_core.at[chip, share],
            part_send.at[chip, share], part_recv.at[chip, share], tok_id(z, other),
        )

    def sum_copy(chip, d):
        share = (mine + d) % shares
        return remote(
            kept_at(chip, share), from_peer.at[chip, mine],
            peer_send.at[chip, d - 1], peer_recv.at[chip, mine], peer_id(share),
        )

    def compute(i, carry):
        @pl.when(i + 1 < chips)
        def _():
            row_wait(chip_at(i + 1), mine, c)
            forward(i + 1)

        chip = chip_at(i)
        for d in range(1, shares):
            share = (mine + d) % shares
            row_wait(chip, share, c)
            if cores > 1:
                core_copy(chip, share).start()
        if cores > 1:
            for share in range(shares):
                row_wait(chip, share, other)
        gate = jnp.zeros((cores * depth, gate_w.shape[-1]), jnp.float32)
        up = gate
        for share in range(shares):
            block = rows[chip, share].reshape(cores * depth, wide)
            gate += jnp.dot(block, gate_w[0, share], preferred_element_type=jnp.float32)
            up += jnp.dot(block, gate_w[1, share], preferred_element_type=jnp.float32)
        active = (gate * jax.nn.sigmoid(1.702 * gate) * (up + 1.0)).astype(jnp.bfloat16)
        ends = rows[chip, 0, :, :, tail:].reshape(cores * depth, wide - tail).astype(jnp.float32)
        weight = jnp.sum(jnp.where(weight_lane, ends, 0.0), axis=1, keepdims=True)
        for share in range(shares):
            out = jnp.dot(active, down_w[share], preferred_element_type=jnp.float32)
            out = (out * weight).astype(jnp.bfloat16)
            part[chip, share] = out.reshape(cores, depth, width)
            if cores > 1:
                part_copy(chip, share).start()
        for share in range(shares):
            if cores > 1:
                part_copy(chip, share).wait_recv()
                total = part[chip, share, c].astype(jnp.float32)
                total += from_core[chip, share].astype(jnp.float32)
                kept[chip, share] = total.astype(jnp.bfloat16)
        for d in range(1, shares):
            sum_copy(chip, d).start()
        return carry

    lax.fori_loop(0, chips, compute, 0)

    def right_hop(chip):
        return remote(
            hop.at[chip], from_left.at[chip], hop_send.at[chip], left_recv.at[chip],
            tok_id(z + 1, c),
        )

    def left_hop(chip):
        return remote(
            hop.at[chip], from_right.at[chip], hop_send.at[chip], right_recv.at[chip],
            tok_id(z - 1, c),
        )

    def hop_wait(buffer, sem, chip):
        pltpu.make_async_copy(buffer.at[chip], buffer.at[chip], sem.at[chip]).wait()

    def give_back(j, carry):
        chip = chip_at(chips - 1 - j)
        total = kept_at(chip, mine)[...].astype(jnp.float32)
        for d in range(1, shares):
            share = (mine + d) % shares
            slot = from_peer.at[chip, share]
            pltpu.make_async_copy(slot, slot, peer_recv.at[chip, share]).wait()
            total += from_peer[chip, share].astype(jnp.float32)
        out_ref[...] = total

        @pl.when((chip <= z) & (z < chips - 1))
        def _():
            hop_wait(from_right, right_recv, chip)
            out_ref[...] += from_right[chip].astype(jnp.float32)

        @pl.when((chip >= z) & (z > 0))
        def _():
            hop_wait(from_left, left_recv, chip)
            out_ref[...] += from_left[chip].astype(jnp.float32)

        @pl.when(chip != z)
        def _():
            hop[chip] = out_ref[...].astype(jnp.bfloat16)

        @pl.when(chip < z)
        def _():
            left_hop(chip).start()

        @pl.when(chip > z)
        def _():
            right_hop(chip).start()

        return carry

    lax.fori_loop(0, chips, give_back, 0)

    def drain(chip, carry):
        @pl.when(go_right(chip))
        def _():
            right_copy(chip).wait_send()

        @pl.when(go_left(chip))
        def _():
            left_copy(chip).wait_send()

        for d in range(1, shares):
            peer_copy(chip, d).wait_send()
            sum_copy(chip, d).wait_send()
        if cores > 1:
            for share in range(shares):
                core_copy(chip, share).wait_send()
                part_copy(chip, share).wait_send()

        @pl.when(chip < z)
        def _():
            left_hop(chip).wait_send()

        @pl.when(chip > z)
        def _():
            right_hop(chip).wait_send()

        return carry

    lax.fori_loop(0, chips, drain, 0)


def moe(dims, own_rows, gate_w, down_w):
    chips, cores, shares, pairs, width = dims
    depth, wide = own_rows.shape
    hidden = down_w.shape[1]
    bf16 = jnp.bfloat16
    dma = pltpu.SemaphoreType.DMA
    return pl.pallas_call(
        functools.partial(moe_kernel, dims),
        out_shape=jax.ShapeDtypeStruct((depth, width), jnp.float32),
        in_specs=[
            pl.BlockSpec(memory_space=pltpu.VMEM),
            pl.BlockSpec(memory_space=pl.ANY),
            pl.BlockSpec(memory_space=pl.ANY),
        ],
        out_specs=pl.BlockSpec(memory_space=pltpu.VMEM),
        scratch_shapes=[
            pltpu.VMEM(gate_w.shape, bf16),
            pltpu.VMEM(down_w.shape, bf16),
            pltpu.VMEM((chips, shares, cores, depth, wide), bf16),
            pltpu.VMEM((chips, shares, cores, depth, width), bf16),
            pltpu.VMEM((chips, shares, depth, width) if cores > 1 else (8, 128), bf16),
            pltpu.VMEM((chips, shares, depth, width) if cores > 1 else (8, 128), bf16),
            pltpu.VMEM((chips, shares, depth, width), bf16),
            pltpu.VMEM((chips, depth, width), bf16),
            pltpu.VMEM((chips, depth, width), bf16),
            pltpu.VMEM((chips, depth, width), bf16),
            dma((3,)),
            dma((chips, cores, shares)),
            dma((chips,)),
            dma((chips,)),
            dma((chips, max(shares - 1, 1))),
            dma((chips, shares)),
            dma((chips, shares)),
            dma((chips, shares)),
            dma((chips, max(shares - 1, 1))),
            dma((chips, shares)),
            dma((chips,)),
            dma((chips,)),
            dma((chips,)),
        ],
        compiler_params=pltpu.CompilerParams(
            collective_id=0, has_side_effects=True, vmem_limit_bytes=60 * 1024 * 1024
        ),
        cost_estimate=pl.CostEstimate(
            flops=6 * chips * cores * depth * shares * width * hidden,
            bytes_accessed=6 * shares * width * hidden,
            transcendentals=0,
        ),
    )(own_rows, gate_w, down_w)


def per_device(
    queries,
    keys_values,
    sink_logits,
    residual,
    out_weight,
    norm_gain,
    expert_ids,
    route_weights,
    gate_up,
    down_weight,
):
    tok_rows = queries.shape[0]
    kv_groups = keys_values.shape[1] // (2 * HEAD_DIM)
    local_heads = queries.shape[1] // HEAD_DIM
    repeat = local_heads // kv_groups
    position = lax.axis_index("tok") * tok_rows + jnp.arange(tok_rows, dtype=jnp.int32)
    grouped = queries.reshape(tok_rows, kv_groups, repeat, HEAD_DIM)
    start_max = jnp.broadcast_to(
        sink_logits.reshape(kv_groups, repeat)[:, :, None], (kv_groups, repeat, tok_rows)
    )
    start_totals = jnp.ones((kv_groups, repeat, tok_rows), jnp.float32)
    start_accum = jnp.zeros((kv_groups, repeat, tok_rows, HEAD_DIM), jnp.float32)
    key_piece = lax.all_gather(keys_values, "tok", axis=0, tiled=True)
    totals = start_totals
    accum = start_accum
    count = key_piece.shape[0]
    split_piece = key_piece.reshape(count, kv_groups, 2, HEAD_DIM)
    scores = (
        jnp.einsum(
            "tgrd,ngd->grtn", grouped, split_piece[:, :, 0], preferred_element_type=jnp.float32
        )
        * 0.125
    )
    key_position = jnp.arange(count, dtype=jnp.int32)
    allowed = key_position[None, :] <= position[:, None]
    scores = jnp.where(allowed, scores, jnp.float32(-1e30))
    new_max = jnp.maximum(start_max, jnp.max(scores, axis=-1))
    decay = jnp.exp(start_max - new_max)
    weights = jnp.exp(scores - new_max[..., None])
    totals = totals * decay + jnp.sum(weights, axis=-1)
    update = jnp.einsum(
        "grtn,ngd->grtd",
        weights.astype(jnp.bfloat16),
        split_piece[:, :, 1],
        preferred_element_type=jnp.float32,
    )
    accum = accum * decay[..., None] + update
    final_max, totals, accum = (new_max, totals, accum)
    attended = (accum / totals[..., None]).astype(jnp.bfloat16)
    attended = jnp.transpose(attended, (2, 0, 1, 3)).reshape(tok_rows, local_heads * HEAD_DIM)
    width = out_weight.shape[1]
    share = width // lax.axis_size(("head", "pair"))
    column_start = lax.axis_index(("head", "pair")) * share
    partial_value = jnp.dot(attended, out_weight, preferred_element_type=jnp.float32)
    projected = lax.psum(partial_value.astype(jnp.bfloat16), ("head", "pair")).astype(jnp.float32)
    stream = residual.astype(jnp.float32) + projected
    inverse = lax.rsqrt(jnp.mean(stream * stream, axis=-1, keepdims=True) + 1e-05)
    normed = (stream * inverse * norm_gain).astype(jnp.bfloat16)
    experts = lax.axis_size("tok")
    pairs = lax.axis_size("pair")
    cores = 2 // pairs
    shares = width // share
    hidden = down_weight.shape[1]
    wide = -(-(share + 2 * experts) // 128) * 128
    expert = jnp.arange(experts, dtype=jnp.int32)
    routed = expert_ids[:, :, None] == expert
    dense = jnp.sum(jnp.where(routed, route_weights[:, :, None], 0.0), axis=1)
    high = lax.reduce_precision(dense, 8, 7)
    own_rows = jnp.concatenate(
        [
            lax.dynamic_slice_in_dim(normed, column_start, share, 1),
            high.astype(jnp.bfloat16),
            (dense - high).astype(jnp.bfloat16),
            jnp.zeros((tok_rows, wide - share - 2 * experts), jnp.bfloat16),
        ],
        axis=1,
    )
    gate_w = jnp.transpose(gate_up[0], (1, 0, 2)).reshape(2, shares, share, hidden)
    gate_w = jnp.pad(gate_w, ((0, 0), (0, 0), (0, wide - share), (0, 0)))
    down_w = jnp.transpose(down_weight[0].reshape(hidden, shares, share), (1, 0, 2))
    stream_share = lax.dynamic_slice_in_dim(stream, column_start, share, 1)
    mixture = moe((experts // cores, cores, shares, pairs, share), own_rows, gate_w, down_w)
    return (stream_share + mixture).astype(jnp.bfloat16)


def solution(mesh):
    placed = (
        P(("groups", "tok"), ("head", "pair")),
        P(("groups", "tok"), ("head", "pair")),
        P(("head", "pair")),
        P(("groups", "tok"), None),
        P(("head", "pair"), None),
        P(),
        P(("groups", "tok"), None),
        P(("groups", "tok"), None),
        P("tok", None, None, ("head", "pair")),
        P("tok", ("head", "pair"), None),
    )
    return jax.shard_map(
        per_device,
        mesh=mesh,
        in_specs=placed,
        out_specs=P(("groups", "tok"), ("head", "pair")),
        check_vma=False,
    )
```

```python
import functools

import jax
import jax.numpy as jnp
from jax import lax
from jax.experimental import pallas as pl
from jax.experimental.pallas import tpu as pltpu
from jax.sharding import PartitionSpec as P

HEAD_DIM = 64

MESH_ID = pl.DeviceIdType.MESH


def moe_kernel(
    dims,
    parts_ref,
    residual_ref,
    gain_ref,
    tail_ref,
    gate_hbm,
    down_hbm,
    out_ref,
    gate_w,
    down_w,
    rows,
    part,
    from_core,
    kept,
    from_peer,
    hop,
    from_right,
    from_left,
    peer_parts,
    stream,
    squares,
    peer_squares,
    acc,
    parts_send,
    parts_recv,
    squares_send,
    squares_recv,
    load_sem,
    row_recv,
    row_right,
    row_left,
    row_peer,
    row_core,
    part_send,
    part_recv,
    peer_send,
    peer_recv,
    hop_send,
    right_recv,
    left_recv,
):
    chips, cores, shares, pairs, width = dims
    tok = lax.axis_index("tok")
    z = tok // cores
    c = tok % cores
    mine = lax.axis_index("head") * pairs + lax.axis_index("pair")
    other = cores - 1 - c

    def tok_id(chip, core):
        return {"tok": chip * cores + core}

    def peer_id(share):
        return {"head": share // pairs, "pair": share % pairs}

    def remote(src, dst, send, recv, target):
        return pltpu.make_async_remote_copy(
            src_ref=src, dst_ref=dst, send_sem=send, recv_sem=recv,
            device_id=target, device_id_type=MESH_ID,
        )

    loads = [
        pltpu.make_async_copy(gate_hbm, gate_w.at[:, :, pl.ds(0, width)], load_sem.at[0]),
        pltpu.make_async_copy(down_hbm, down_w, load_sem.at[1]),
    ]
    for load in loads:
        load.start()

    barrier = pltpu.get_barrier_semaphore()

    @pl.when(z > 0)
    def _():
        pl.semaphore_signal(barrier, 1, device_id=tok_id(z - 1, c), device_id_type=MESH_ID)

    @pl.when(z < chips - 1)
    def _():
        pl.semaphore_signal(barrier, 1, device_id=tok_id(z + 1, c), device_id_type=MESH_ID)

    if cores > 1:
        pl.semaphore_signal(barrier, 1, device_id=tok_id(z, other), device_id_type=MESH_ID)
    for d in range(1, shares):
        pl.semaphore_signal(
            barrier, 1, device_id=peer_id((mine + d) % shares), device_id_type=MESH_ID
        )
    sides = jnp.where(z > 0, 1, 0) + jnp.where(z < chips - 1, 1, 0)
    pl.semaphore_wait(barrier, sides + (cores - 1) + (shares - 1))

    def parts_copy(d):
        share = (mine + d) % shares
        return remote(
            parts_ref.at[share], peer_parts.at[mine], parts_send.at[d - 1],
            parts_recv.at[mine], peer_id(share),
        )

    def squares_copy(d):
        return remote(
            squares, peer_squares.at[mine], squares_send.at[d - 1],
            squares_recv.at[mine], peer_id((mine + d) % shares),
        )

    for d in range(1, shares):
        parts_copy(d).start()
    gate_w[:, :, width:, :] = jnp.zeros(
        gate_w.shape[:2] + (gate_w.shape[2] - width, gate_w.shape[3]), jnp.bfloat16
    )
    stream[...] = residual_ref[...].astype(jnp.float32) + parts_ref[mine].astype(jnp.float32)
    for d in range(1, shares):
        share = (mine + d) % shares
        slot = peer_parts.at[share]
        pltpu.make_async_copy(slot, slot, parts_recv.at[share]).wait()
        stream[...] += peer_parts[share].astype(jnp.float32)
    own = stream[...]
    square = jnp.sum(own * own, axis=1, keepdims=True)
    squares[...] = jnp.broadcast_to(square, squares.shape)
    for d in range(1, shares):
        squares_copy(d).start()
    total_square = squares[...]
    for d in range(1, shares):
        share = (mine + d) % shares
        slot = peer_squares.at[share]
        pltpu.make_async_copy(slot, slot, squares_recv.at[share]).wait()
        total_square += peer_squares[share]
    inverse = lax.rsqrt(total_square[:, :1] / (shares * width) + 1e-05)
    normed = stream[...] * inverse * gain_ref[...] + tail_ref[...].astype(jnp.float32)
    rows[z, mine, c] = normed.astype(jnp.bfloat16)

    near = jnp.minimum(z, chips - 1 - z)

    def chip_at(i):
        inner = jnp.where(i % 2 == 1, z - (i + 1) // 2, z + i // 2)
        outer = jnp.where(z < chips - 1 - z, i, chips - 1 - i)
        return jnp.where(i <= 2 * near, inner, outer)

    def row_copy(chip, share, core, send, target):
        slot = rows.at[chip, share, core]
        return remote(slot, slot, send, row_recv.at[chip, core, share], target)

    def go_right(chip):
        return (chip <= z) & (z < chips - 1)

    def go_left(chip):
        return (chip >= z) & (z > 0)

    def right_copy(chip):
        return row_copy(chip, mine, c, row_right.at[chip], tok_id(z + 1, c))

    def left_copy(chip):
        return row_copy(chip, mine, c, row_left.at[chip], tok_id(z - 1, c))

    def peer_copy(chip, d):
        return row_copy(chip, mine, c, row_peer.at[chip, d - 1], peer_id((mine + d) % shares))

    def core_copy(chip, share):
        return row_copy(chip, share, c, row_core.at[chip, share], tok_id(z, other))

    def row_wait(chip, share, core):
        slot = rows.at[chip, share, core]
        pltpu.make_async_copy(slot, slot, row_recv.at[chip, core, share]).wait()

    def forward(i):
        chip = chip_at(i)

        @pl.when(go_right(chip))
        def _():
            right_copy(chip).start()

        @pl.when(go_left(chip))
        def _():
            left_copy(chip).start()

        for d in range(1, shares):
            peer_copy(chip, d).start()
        if cores > 1:
            core_copy(chip, mine).start()

    forward(0)
    loads[0].wait()
    loads[1].wait()

    tail = (width // 128) * 128
    wide = rows.shape[-1]
    depth = rows.shape[-2]
    experts = chips * cores
    tail_lane = tail + lax.broadcasted_iota(jnp.int32, (cores * depth, wide - tail), 1)
    weight_lane = (tail_lane == width + tok) | (tail_lane == width + experts + tok)

    def kept_at(chip, share):
        return kept.at[chip, share] if cores > 1 else part.at[chip, share, 0]

    def part_copy(chip, share):
        return remote(
            part.at[chip, share, other], from_core.at[chip, share],
            part_send.at[chip, share], part_recv.at[chip, share], tok_id(z, other),
        )

    def sum_copy(chip, d):
        share = (mine + d) % shares
        return remote(
            kept_at(chip, share), from_peer.at[chip, mine],
            peer_send.at[chip, d - 1], peer_recv.at[chip, mine], peer_id(share),
        )

    def compute(i, carry):
        @pl.when(i + 1 < chips)
        def _():
            row_wait(chip_at(i + 1), mine, c)
            forward(i + 1)

        chip = chip_at(i)
        for d in range(1, shares):
            share = (mine + d) % shares
            row_wait(chip, share, c)
            if cores > 1:
                core_copy(chip, share).start()
        if cores > 1:
            for share in range(shares):
                row_wait(chip, share, other)
        gate = jnp.zeros((cores * depth, gate_w.shape[-1]), jnp.float32)
        up = gate
        for share in range(shares):
            block = rows[chip, share].reshape(cores * depth, wide)
            gate += jnp.dot(block, gate_w[0, share], preferred_element_type=jnp.float32)
            up += jnp.dot(block, gate_w[1, share], preferred_element_type=jnp.float32)
        active = (gate * jax.nn.sigmoid(1.702 * gate) * (up + 1.0)).astype(jnp.bfloat16)
        ends = rows[chip, 0, :, :, tail:].reshape(cores * depth, wide - tail).astype(jnp.float32)
        weight = jnp.sum(jnp.where(weight_lane, ends, 0.0), axis=1, keepdims=True)
        for share in range(shares):
            out = jnp.dot(active, down_w[share], preferred_element_type=jnp.float32)
            out = (out * weight).astype(jnp.bfloat16)
            part[chip, share] = out.reshape(cores, depth, width)
            if cores > 1:
                part_copy(chip, share).start()
        for share in range(shares):
            if cores > 1:
                part_copy(chip, share).wait_recv()
                total = part[chip, share, c].astype(jnp.float32)
                total += from_core[chip, share].astype(jnp.float32)
                kept[chip, share] = total.astype(jnp.bfloat16)
        for d in range(1, shares):
            sum_copy(chip, d).start()
        return carry

    lax.fori_loop(0, chips, compute, 0)

    def right_hop(chip):
        return remote(
            hop.at[chip], from_left.at[chip], hop_send.at[chip], left_recv.at[chip],
            tok_id(z + 1, c),
        )

    def left_hop(chip):
        return remote(
            hop.at[chip], from_right.at[chip], hop_send.at[chip], right_recv.at[chip],
            tok_id(z - 1, c),
        )

    def hop_wait(buffer, sem, chip):
        pltpu.make_async_copy(buffer.at[chip], buffer.at[chip], sem.at[chip]).wait()

    def give_back(j, carry):
        chip = chip_at(chips - 1 - j)
        total = kept_at(chip, mine)[...].astype(jnp.float32)
        for d in range(1, shares):
            share = (mine + d) % shares
            slot = from_peer.at[chip, share]
            pltpu.make_async_copy(slot, slot, peer_recv.at[chip, share]).wait()
            total += from_peer[chip, share].astype(jnp.float32)
        acc[...] = total

        @pl.when((chip <= z) & (z < chips - 1))
        def _():
            hop_wait(from_right, right_recv, chip)
            acc[...] += from_right[chip].astype(jnp.float32)

        @pl.when((chip >= z) & (z > 0))
        def _():
            hop_wait(from_left, left_recv, chip)
            acc[...] += from_left[chip].astype(jnp.float32)

        @pl.when(chip == z)
        def _():
            out_ref[...] = (stream[:, :width] + acc[...]).astype(jnp.bfloat16)

        @pl.when(chip != z)
        def _():
            hop[chip] = acc[...].astype(jnp.bfloat16)

        @pl.when(chip < z)
        def _():
            left_hop(chip).start()

        @pl.when(chip > z)
        def _():
            right_hop(chip).start()

        return carry

    lax.fori_loop(0, chips, give_back, 0)

    def drain(chip, carry):
        @pl.when(go_right(chip))
        def _():
            right_copy(chip).wait_send()

        @pl.when(go_left(chip))
        def _():
            left_copy(chip).wait_send()

        for d in range(1, shares):
            peer_copy(chip, d).wait_send()
            sum_copy(chip, d).wait_send()
        if cores > 1:
            for share in range(shares):
                core_copy(chip, share).wait_send()
                part_copy(chip, share).wait_send()

        @pl.when(chip < z)
        def _():
            left_hop(chip).wait_send()

        @pl.when(chip > z)
        def _():
            right_hop(chip).wait_send()

        return carry

    lax.fori_loop(0, chips, drain, 0)
    for d in range(1, shares):
        parts_copy(d).wait_send()
        squares_copy(d).wait_send()


def moe(dims, parts, residual, gain, tail, gate_w, down_w):
    chips, cores, shares, pairs, width = dims
    depth, wide = residual.shape
    hidden = down_w.shape[1]
    bf16 = jnp.bfloat16
    dma = pltpu.SemaphoreType.DMA
    return pl.pallas_call(
        functools.partial(moe_kernel, dims),
        out_shape=jax.ShapeDtypeStruct((depth, width), jnp.bfloat16),
        in_specs=[pl.BlockSpec(memory_space=pltpu.VMEM)] * 4
        + [
            pl.BlockSpec(memory_space=pl.ANY),
            pl.BlockSpec(memory_space=pl.ANY),
        ],
        out_specs=pl.BlockSpec(memory_space=pltpu.VMEM),
        scratch_shapes=[
            pltpu.VMEM((2, shares, wide, hidden), bf16),
            pltpu.VMEM(down_w.shape, bf16),
            pltpu.VMEM((chips, shares, cores, depth, wide), bf16),
            pltpu.VMEM((chips, shares, cores, depth, width), bf16),
            pltpu.VMEM((chips, shares, depth, width) if cores > 1 else (8, 128), bf16),
            pltpu.VMEM((chips, shares, depth, width) if cores > 1 else (8, 128), bf16),
            pltpu.VMEM((chips, shares, depth, width), bf16),
            pltpu.VMEM((chips, depth, width), bf16),
            pltpu.VMEM((chips, depth, width), bf16),
            pltpu.VMEM((chips, depth, width), bf16),
            pltpu.VMEM((shares, depth, wide), bf16),
            pltpu.VMEM((depth, wide), jnp.float32),
            pltpu.VMEM((depth, 128), jnp.float32),
            pltpu.VMEM((shares, depth, 128), jnp.float32),
            pltpu.VMEM((depth, width), jnp.float32),
            dma((max(shares - 1, 1),)),
            dma((shares,)),
            dma((max(shares - 1, 1),)),
            dma((shares,)),
            dma((2,)),
            dma((chips, cores, shares)),
            dma((chips,)),
            dma((chips,)),
            dma((chips, max(shares - 1, 1))),
            dma((chips, shares)),
            dma((chips, shares)),
            dma((chips, shares)),
            dma((chips, max(shares - 1, 1))),
            dma((chips, shares)),
            dma((chips,)),
            dma((chips,)),
            dma((chips,)),
        ],
        compiler_params=pltpu.CompilerParams(
            collective_id=0, has_side_effects=True, vmem_limit_bytes=60 * 1024 * 1024
        ),
        cost_estimate=pl.CostEstimate(
            flops=6 * chips * cores * depth * shares * width * hidden,
            bytes_accessed=6 * shares * width * hidden,
            transcendentals=0,
        ),
    )(parts, residual, gain, tail, gate_w, down_w)


def per_device(
    queries,
    keys_values,
    sink_logits,
    residual,
    out_weight,
    norm_gain,
    expert_ids,
    route_weights,
    gate_up,
    down_weight,
):
    tok_rows = queries.shape[0]
    kv_groups = keys_values.shape[1] // (2 * HEAD_DIM)
    local_heads = queries.shape[1] // HEAD_DIM
    repeat = local_heads // kv_groups
    position = lax.axis_index("tok") * tok_rows + jnp.arange(tok_rows, dtype=jnp.int32)
    grouped = queries.reshape(tok_rows, kv_groups, repeat, HEAD_DIM)
    start_max = jnp.broadcast_to(
        sink_logits.reshape(kv_groups, repeat)[:, :, None], (kv_groups, repeat, tok_rows)
    )
    start_totals = jnp.ones((kv_groups, repeat, tok_rows), jnp.float32)
    start_accum = jnp.zeros((kv_groups, repeat, tok_rows, HEAD_DIM), jnp.float32)
    key_piece = lax.all_gather(keys_values, "tok", axis=0, tiled=True)
    hidden = down_weight.shape[1]
    shares = lax.axis_size(("head", "pair"))
    share = out_weight.shape[1] // shares
    gate_w = jnp.transpose(gate_up[0], (1, 0, 2)).reshape(2, shares, share, hidden)
    down_w = jnp.transpose(down_weight[0].reshape(hidden, shares, share), (1, 0, 2))
    key_piece, gate_w, down_w = lax.optimization_barrier((key_piece, gate_w, down_w))
    totals = start_totals
    accum = start_accum
    count = key_piece.shape[0]
    split_piece = key_piece.reshape(count, kv_groups, 2, HEAD_DIM)
    scores = (
        jnp.einsum(
            "tgrd,ngd->grtn", grouped, split_piece[:, :, 0], preferred_element_type=jnp.float32
        )
        * 0.125
    )
    key_position = jnp.arange(count, dtype=jnp.int32)
    allowed = key_position[None, :] <= position[:, None]
    scores = jnp.where(allowed, scores, jnp.float32(-1e30))
    new_max = jnp.maximum(start_max, jnp.max(scores, axis=-1))
    decay = jnp.exp(start_max - new_max)
    weights = jnp.exp(scores - new_max[..., None])
    totals = totals * decay + jnp.sum(weights, axis=-1)
    update = jnp.einsum(
        "grtn,ngd->grtd",
        weights.astype(jnp.bfloat16),
        split_piece[:, :, 1],
        preferred_element_type=jnp.float32,
    )
    accum = accum * decay[..., None] + update
    final_max, totals, accum = (new_max, totals, accum)
    attended = (accum / totals[..., None]).astype(jnp.bfloat16)
    attended = jnp.transpose(attended, (2, 0, 1, 3)).reshape(tok_rows, local_heads * HEAD_DIM)
    width = out_weight.shape[1]
    share = width // lax.axis_size(("head", "pair"))
    column_start = lax.axis_index(("head", "pair")) * share
    partial_value = jnp.dot(attended, out_weight, preferred_element_type=jnp.float32)
    experts = lax.axis_size("tok")
    pairs = lax.axis_size("pair")
    cores = 2 // pairs
    shares = width // share
    wide = -(-(share + 2 * experts) // 128) * 128
    expert = jnp.arange(experts, dtype=jnp.int32)
    routed = expert_ids[:, :, None] == expert
    dense = jnp.sum(jnp.where(routed, route_weights[:, :, None], 0.0), axis=1)
    high = lax.reduce_precision(dense, 8, 7)
    weights = jnp.concatenate([high, dense - high], axis=1).astype(jnp.bfloat16)
    tail = jnp.pad(weights, ((0, 0), (share, wide - share - 2 * experts)))
    spare = (0, wide - share)
    parts = jnp.transpose(
        partial_value.astype(jnp.bfloat16).reshape(tok_rows, shares, share), (1, 0, 2)
    )
    parts = jnp.pad(parts, ((0, 0), (0, 0), spare))
    own_residual = jnp.pad(
        lax.dynamic_slice_in_dim(residual, column_start, share, 1), ((0, 0), spare)
    )
    own_gain = jnp.pad(lax.dynamic_slice_in_dim(norm_gain, column_start, share, 0), spare)
    return moe(
        (experts // cores, cores, shares, pairs, share),
        parts, own_residual, own_gain[None, :], tail, gate_w, down_w,
    )


def solution(mesh):
    placed = (
        P(("groups", "tok"), ("head", "pair")),
        P(("groups", "tok"), ("head", "pair")),
        P(("head", "pair")),
        P(("groups", "tok"), None),
        P(("head", "pair"), None),
        P(),
        P(("groups", "tok"), None),
        P(("groups", "tok"), None),
        P("tok", None, None, ("head", "pair")),
        P("tok", ("head", "pair"), None),
    )
    return jax.shard_map(
        per_device,
        mesh=mesh,
        in_specs=placed,
        out_specs=P(("groups", "tok"), ("head", "pair")),
        check_vma=False,
    )
```
